8 devices in a mesh: dp: 1 (over z), tp: 8 (over x, y, core).
Axes of the slice: x: 2, y: 2, z: 1, core: 2. Of those that a mesh axis runs over, the one named last changes fastest.
Arguments:
- x: bfloat16 [2048, 8192], P('dp')
- gain: bfloat16 [8192], replicated
- wq: bfloat16 [8192, 8192], P(None, 'tp')
- wk: bfloat16 [8192, 8192], P(None, 'tp')
- wv: bfloat16 [8192, 8192], P(None, 'tp')
- wo: bfloat16 [8192, 8192], P('tp')
Outputs:
- output: bfloat16 [2048, 8192], P('dp')
All inputs are finite; a program needn't handle non-finite values.
Results may differ from the reference program's by a relative error of at most 0.012.
Values are sent between devices in bfloat16 or wider.
A program may use at most 2 GiB of HBM per device.

```python
import jax
import jax.numpy as jnp
from jax import lax

ROWS = 2048
D = 8192
HEADS = 64
KV_HEADS = 64
HEAD = 128
THETA = 10000


def setup_inputs(seed: int = 0, part: int = 0) -> dict:
    kx, kn, kq, kk, kv, ko = jax.random.split(jax.random.key(seed), 6)

    def weights(key, rows, columns):
        return jax.random.normal(key, (rows, columns), jnp.float32) * rows**-0.5

    drawn = {
        "x": jax.random.normal(jax.random.fold_in(kx, part), (ROWS, D), jnp.float32),
        "gain": 1 + 0.1 * jax.random.normal(kn, (D,), jnp.float32),
        "wq": 2 * weights(kq, D, HEADS * HEAD),
        "wk": 2 * weights(kk, D, KV_HEADS * HEAD),
        "wv": 4 * weights(kv, D, KV_HEADS * HEAD),
        "wo": weights(ko, HEADS * HEAD, D),
    }
    return {k: v.astype(jnp.bfloat16) for k, v in drawn.items()}


def normed(x, gain):
    wide = x.astype(jnp.float32)
    scale = lax.rsqrt(jnp.mean(wide * wide, -1, keepdims=True) + 1e-6)
    return (wide * scale * gain.astype(jnp.float32)).astype(jnp.bfloat16)


def turned(t, place, theta):
    half = t.shape[-1] // 2
    angle = place.astype(jnp.float32)[:, None] * theta ** (-jnp.arange(half, dtype=jnp.float32) / half)
    cos, sin = jnp.cos(angle)[:, None], jnp.sin(angle)[:, None]
    a, b = t[..., :half].astype(jnp.float32), t[..., half:].astype(jnp.float32)
    return jnp.concatenate([a * cos - b * sin, b * cos + a * sin], -1).astype(jnp.bfloat16)


def matmul(a, w):
    return jnp.dot(a, w, preferred_element_type=jnp.float32).astype(jnp.bfloat16)


def einsum(form, a, b):
    return jnp.einsum(form, a.astype(jnp.float32), b.astype(jnp.float32))


def attention(q, k, v):
    scores = einsum("tgsd,ugd->gstu", q, k) * q.shape[-1] ** -0.5
    token = jnp.arange(q.shape[0])
    scores = jnp.where(token[:, None] >= token, scores, -jnp.inf)
    weights = jax.nn.softmax(scores, -1).astype(jnp.bfloat16)
    return einsum("gstu,ugd->tgsd", weights, v).astype(jnp.bfloat16)


def reference(x, gain, wq, wk, wv, wo):
    a, place = normed(x, gain), jnp.arange(ROWS)
    q = turned(matmul(a, wq).reshape(ROWS, HEADS, HEAD), place, THETA).reshape(ROWS, KV_HEADS, -1, HEAD)
    k = turned(matmul(a, wk).reshape(ROWS, KV_HEADS, HEAD), place, THETA)
    v = matmul(a, wv).reshape(ROWS, KV_HEADS, HEAD)
    seen = attention(q, k, v).reshape(ROWS, HEADS * HEAD)
    return (x.astype(jnp.float32) + jnp.dot(seen, wo, preferred_element_type=jnp.float32)).astype(jnp.bfloat16)
```

```python
import functools

import jax
import jax.numpy as jnp
import numpy as np
from jax import lax
from jax.experimental import pallas as pl
from jax.experimental.pallas import tpu as pltpu
from jax.sharding import PartitionSpec as P

HEAD = 128
THETA = 10000
NEG = -1e30
HIDDEN = 2 * NEG
LOG2E = 1.4426950408889634
MESH = pl.DeviceIdType.MESH
F32, BF16 = jnp.float32, jnp.bfloat16

R = 256
WT = 256
NQ = 3
NW = 3


def tables(rows):
    half = HEAD // 2
    rate = np.power(np.float32(THETA), -np.arange(half, dtype=np.float32) / np.float32(half)).astype(np.float32)
    angle = np.arange(rows, dtype=np.float32)[:, None] * rate
    cos, sin = np.cos(angle), np.sin(angle)
    return np.concatenate([cos, cos], 1).astype(np.float32), np.concatenate([-sin, sin], 1).astype(np.float32)


def kernel(x_ref, gain_ref, cos_ref, sin_ref, wq_ref, wk_ref, wv_ref, wo_ref, y_ref,
           xa, cos_s, sin_s, ring, wring, q_s, k_s, v_s, seen, top_s, mix_s,
           dsend, drecv, p1send, p1recv, p2send, p2recv, acc, fin, xres,
           x_sem, t_sem, ring_sem, wring_sem, xres_sem,
           d_ss, d_rs, p1_ss, p1_rs, p2_ss, p2_rs, p3_ss, p3_rs, p4_ss, p4_rs, p4f_ss, p4f_rs,
           loc_sem, e2_ss, e3_ss, e4_ss, e_rs):
    rows, width = x_ref.shape
    nc = rows // R
    heads = q_s.shape[0]
    cols = heads * HEAD
    half = width // 2
    tile = half // 4
    piece = tile // 2
    tiles = cols // WT

    me = lax.axis_index("tp")
    core, yy, xx = lax.rem(me, 2), lax.rem(me // 2, 2), me // 4
    mate = me + 1 - 2 * core
    ypeer = me + 2 - 4 * yy
    xpeer = me + 4 - 8 * xx
    peers = (xpeer, ypeer)
    cross = (ypeer, xpeer)

    def remote(src, dst, ss, rs, to):
        return pltpu.make_async_remote_copy(src, dst, ss, rs, device_id={"tp": to}, device_id_type=MESH)

    def column(h, kind, s):
        a = kind % 2 == 0
        lead, other = (xx, yy) if a else (yy, xx)
        big = 1 - lead if kind < 2 else lead
        small = other if s == 0 else 1 - other
        return pl.multiple_of(h * half + (0 if a else 2 * tile) + big * tile + small * piece, piece)

    def at_rows(c):
        return pl.ds(pl.multiple_of(c * R, R), R)

    def x_copy(c):
        p = lax.rem(c, 2)
        return pltpu.make_async_copy(x_ref.at[at_rows(c)], xa.at[p], x_sem.at[p])

    def issue_tile(g):
        slot, kind, t = lax.rem(g, NQ), lax.rem(g // tiles, 3), lax.rem(g, tiles)
        for n, w in enumerate((wq_ref, wk_ref, wv_ref)):
            @pl.when(kind == n)
            def _():
                pltpu.make_async_copy(w.at[:, pl.ds(pl.multiple_of(t * WT, WT), WT)], ring.at[slot], ring_sem.at[slot]).start()

    def wo_copies(n, slot):
        h = 1 - core if n < 4 else core
        return [pltpu.make_async_copy(wo_ref.at[:, pl.ds(column(h, n % 4, s), piece)],
                                      wring.at[slot, :, pl.ds(s * piece, piece)], wring_sem.at[slot, s]) for s in range(2)]

    def d_copy(c, k):
        p = lax.rem(c, 2)
        return remote(dsend.at[k], drecv.at[p, k], d_ss.at[k], d_rs.at[p, k], mate)

    def p1_copy(c, k):
        p = lax.rem(c, 2)
        return remote(p1send.at[k], p1recv.at[p, k], p1_ss.at[k], p1_rs.at[p, k], peers[k])

    def p2_copy(c, k):
        p = lax.rem(c, 2)
        return remote(p2send.at[k], p2recv.at[p, k], p2_ss.at[k], p2_rs.at[p, k], cross[k])

    def mine(c, k):
        return y_ref.at[at_rows(c), pl.ds(column(core, 2 + k, 0), piece)]

    def p3_copy(c, k):
        p = lax.rem(c, 2)
        return remote(fin.at[p, k], mine(c, k), p3_ss.at[p, k], p3_rs.at[p, k], cross[k])

    def p4_copy(c, k):
        p = lax.rem(c, 2)
        return remote(fin.at[p, k], mine(c, k), p4_ss.at[p, k], p4_rs.at[p, k], peers[k])

    def e2_copy(c, k):
        p = lax.rem(c, 2)
        return remote(fin.at[p, k], mine(c, k), e2_ss.at[p, k], e_rs, mate)

    def loc_copy(c, k):
        p = lax.rem(c, 2)
        return pltpu.make_async_copy(fin.at[p, k], mine(c, k), loc_sem.at[p, k])

    def came3(c, k):
        return y_ref.at[at_rows(c), pl.ds(column(core, 2 + k, 1), piece)]

    def p4f_copy(c, k):
        p = lax.rem(c, 2)
        return remote(came3(c, k), came3(c, k), p4f_ss.at[p, k], p4f_rs.at[p, k], peers[k])

    def e3_copy(c, k):
        p = lax.rem(c, 2)
        return remote(came3(c, k), came3(c, k), e3_ss.at[p, k], e_rs, mate)

    def e4_copy(c, k):
        p = lax.rem(c, 2)
        lead = xx if k == 0 else yy
        first = pl.multiple_of(core * half + 2 * k * tile + (1 - lead) * tile, tile)
        there = y_ref.at[at_rows(c), pl.ds(first, tile)]
        return remote(there, there, e4_ss.at[p, k], e_rs, mate)

    x_copy(0).start()
    for g in range(NQ):
        issue_tile(jnp.int32(g))
    tab = [pltpu.make_async_copy(cos_ref, cos_s, t_sem.at[0]), pltpu.make_async_copy(sin_ref, sin_s, t_sem.at[1])]
    for t in tab:
        t.start()
    for n in range(NW):
        for copy in wo_copies(n, n):
            copy.start()
    v_s[:, HEAD:, :] = jnp.ones((heads, 8, rows), BF16)
    barrier = pltpu.get_barrier_semaphore()
    for to in (mate, xpeer, ypeer):
        pl.semaphore_signal(barrier, inc=1, device_id={"tp": to}, device_id_type=MESH)
    pl.semaphore_wait(barrier, 3)
    for t in tab:
        t.wait()

    def norm(i):
        p = lax.rem(i, 2)
        x_copy(i).wait()

        @pl.when(i + 1 < nc)
        def _():
            x_copy(i + 1).start()

        def some(b, _):
            at = pl.ds(pl.multiple_of(b * 16, 16), 16)
            wide = xa[p, at, :].astype(F32)
            scale = lax.rsqrt(jnp.mean(wide * wide, -1, keepdims=True) + 1e-6)
            xa[p, at, :] = (wide * scale * gain_ref[...].astype(F32)).astype(BF16)
            return 0

        lax.fori_loop(0, R // 16, some, 0)

    def project(i, first, last):
        p = lax.rem(i, 2)
        here = at_rows(i)

        def one(j, _):
            g = i * (3 * tiles) + j
            slot, kind, t = lax.rem(g, NQ), j // tiles, lax.rem(j, tiles)
            pltpu.make_async_copy(wq_ref.at[:, pl.ds(0, WT)], ring.at[slot], ring_sem.at[slot]).wait()
            out = jnp.dot(xa[p], ring[slot], preferred_element_type=F32).astype(BF16)
            n_head = WT // HEAD

            @pl.when(g + NQ < nc * 3 * tiles)
            def _():
                issue_tile(g + NQ)

            @pl.when(kind == 2)
            def _():
                for n in range(n_head):
                    v_s[t * n_head + n, pl.ds(0, HEAD), here] = out[:, n * HEAD:(n + 1) * HEAD].T

            @pl.when(kind < 2)
            def _():
                cos, sin = cos_s[here, :], sin_s[here, :]
                for n in range(n_head):
                    one_head = out[:, n * HEAD:(n + 1) * HEAD].astype(F32)
                    turned = (one_head * cos + pltpu.roll(one_head, HEAD // 2, 1) * sin).astype(BF16)

                    @pl.when(kind == 0)
                    def _():
                        q_s[t * n_head + n] = turned.T

                    @pl.when(kind == 1)
                    def _():
                        k_s[t * n_head + n, here, :] = turned
            return 0

        lax.fori_loop(first, last, one, 0)

    def attention(i):
        e = HEAD**-0.5 * LOG2E
        for h in range(heads):
            top_s[h:h + 1, :] = jnp.full((1, R), NEG, F32)
            mix_s[h] = jnp.zeros((HEAD + 8, R), F32)

        def block(j, masked):
            here = pl.ds(pl.multiple_of(j * R, R), R)
            scores = [jnp.dot(k_s[h, here, :], q_s[h], preferred_element_type=F32) for h in range(heads)]
            if masked:
                ok = lax.broadcasted_iota(jnp.int32, (R, R), 1) >= lax.broadcasted_iota(jnp.int32, (R, R), 0)
            weights, keeps = [], []
            for h, s in enumerate(scores):
                if masked:
                    s = jnp.where(ok, s, HIDDEN)
                old = top_s[h:h + 1, :]
                top = jnp.maximum(old, s.max(axis=0, keepdims=True))
                top_s[h:h + 1, :] = top
                weights.append(jnp.exp2((s - top) * e).astype(BF16))
                keeps.append(jnp.exp2((old - top) * e))
            for h in range(heads):
                mix_s[h] = mix_s[h] * keeps[h] + jnp.dot(v_s[h, :, here], weights[h], preferred_element_type=F32)

        def whole(j, _):
            block(j, False)
            return 0

        lax.fori_loop(0, i, whole, 0)
        block(i, True)
        for h in range(heads):
            total = mix_s[h, HEAD:HEAD + 1, :]
            seen[:, h * HEAD:(h + 1) * HEAD] = (mix_s[h, :HEAD, :] * (1 / total)).T.astype(BF16)

    def output(i):
        p = lax.rem(i, 2)
        for n in range(8):
            k = n % 4
            slot = lax.rem(i * 8 + n, NW)
            for copy in wo_copies(n, slot):
                copy.wait()
            if n >= 4:
                d_copy(i, k).wait_recv()
            for b in range(tile // 256):
                at = slice(b * 256, (b + 1) * 256)
                out = jnp.dot(seen[...], wring[slot, :, at], preferred_element_type=F32)
                if n < 4:
                    dsend[k, :, at] = out.astype(BF16)
                elif n < 6:
                    p1send[k, :, at] = (out + drecv[p, k, :, at].astype(F32)).astype(BF16)
                else:
                    acc[p, k - 2, :, at] = out + drecv[p, k, :, at].astype(F32)
            after = n + NW
            if after < 8:
                for copy in wo_copies(after, slot):
                    copy.start()
            else:
                @pl.when(i + 1 < nc)
                def _():
                    for copy in wo_copies(after - 8, slot):
                        copy.start()
            if n < 4:
                d_copy(i, k).start()
            elif n < 6:
                p1_copy(i, k).start()

    def xres_copy(c, k):
        return pltpu.make_async_copy(x_ref.at[at_rows(c), pl.ds(column(core, 2 + k, 0), piece)], xres.at[k], xres_sem.at[k])

    def second(c):
        p = lax.rem(c, 2)
        for k in range(4):
            d_copy(c, k).wait_send()
        for k in range(2):
            p1_copy(c, k).wait()
            xres_copy(c, k).start()

            @pl.when(c > 0)
            def _():
                p2_copy(c - 1, k).wait_send()
        for k in range(2):
            p2send[k] = (acc[p, k, :, piece:] + p1recv[p, k, :, piece:].astype(F32)).astype(BF16)
            acc[p, k, :, :piece] = acc[p, k, :, :piece] + p1recv[p, k, :, :piece].astype(F32)
        for k in range(2):
            p2_copy(c, k).start()

    def third(c):
        p = lax.rem(c, 2)

        @pl.when(c >= 2)
        def _():
            done_fin(c - 2)

        for k in range(2):
            p2_copy(c, k).wait_recv()
            xres_copy(c, k).wait()
        for k in range(2):
            fin[p, k] = (acc[p, k, :, :piece] + p2recv[p, k].astype(F32) + xres[k].astype(F32)).astype(BF16)
        for k in range(2):
            p3_copy(c, k).start()
        for k in range(2):
            loc_copy(c, k).start()
            e2_copy(c, k).start()

    def done_fin(c):
        for k in range(2):
            p3_copy(c, k).wait_send()
            p4_copy(c, k).wait_send()
            e2_copy(c, k).wait_send()
            loc_copy(c, k).wait()

    def done_fwd(c):
        for k in range(2):
            p4f_copy(c, k).wait_send()
            e3_copy(c, k).wait_send()

    def forward(c):
        @pl.when(c >= 2)
        def _():
            done_fwd(c - 2)

        for k in range(2):
            p3_copy(c, k).wait_recv()
            p4f_copy(c, k).start()
        for k in range(2):
            e3_copy(c, k).start()

    def last(c):
        @pl.when(c >= 2)
        def _():
            for k in range(2):
                e4_copy(c - 2, k).wait_send()

        for k in range(2):
            p4_copy(c, k).wait_recv()
            p4f_copy(c, k).wait_recv()
            e4_copy(c, k).start()

    def iteration(i, _):
        @pl.when((i >= 2) & (i < nc + 2))
        def _():
            for k in range(2):
                p4_copy(i - 2, k).start()

        @pl.when(i >= 3)
        def _():
            last(i - 3)

        @pl.when(i < nc)
        def _():
            norm(i)
            project(i, 0, 2 * tiles)

        @pl.when((i >= 1) & (i < nc + 1))
        def _():
            second(i - 1)

        @pl.when((i >= 2) & (i < nc + 2))
        def _():
            forward(i - 2)

        @pl.when(i < nc)
        def _():
            project(i, 2 * tiles, 3 * tiles)
            attention(i)

        @pl.when((i >= 1) & (i < nc + 1))
        def _():
            third(i - 1)

        @pl.when(i < nc)
        def _():
            output(i)
        return 0

    lax.fori_loop(0, nc + 3, iteration, 0)

    for k in range(2):
        p2_copy(nc - 1, k).wait_send()
    for c in (nc - 2, nc - 1):
        done_fin(c)
        done_fwd(c)
        for k in range(2):
            e4_copy(c, k).wait_send()
    theirs = y_ref.at[:, pl.ds(pl.multiple_of((1 - core) * half, half), half)]
    remote(theirs, theirs, e2_ss.at[0, 0], e_rs, mate).wait_recv()


def solution(mesh):
    def step(x, gain, wq, wk, wv, wo):
        rows, width = x.shape
        cols = wq.shape[1]
        heads = cols // HEAD
        half, tile, piece = width // 2, width // 8, width // 16
        cos, sin = tables(rows)
        hbm, vmem = pl.BlockSpec(memory_space=pl.ANY), pl.BlockSpec(memory_space=pltpu.VMEM)
        dma = pltpu.SemaphoreType.DMA
        scratch = [
            pltpu.VMEM((2, R, width), BF16),
            pltpu.VMEM((rows, HEAD), F32), pltpu.VMEM((rows, HEAD), F32),
            pltpu.VMEM((NQ, width, WT), BF16), pltpu.VMEM((NW, cols, tile), BF16),
            pltpu.VMEM((heads, HEAD, R), BF16), pltpu.VMEM((heads, rows, HEAD), BF16), pltpu.VMEM((heads, HEAD + 8, rows), BF16),
            pltpu.VMEM((R, cols), BF16), pltpu.VMEM((heads, R), F32), pltpu.VMEM((heads, HEAD + 8, R), F32),
            pltpu.VMEM((4, R, tile), BF16), pltpu.VMEM((2, 4, R, tile), BF16),
            pltpu.VMEM((2, R, tile), BF16), pltpu.VMEM((2, 2, R, tile), BF16),
            pltpu.VMEM((2, R, piece), BF16), pltpu.VMEM((2, 2, R, piece), BF16),
            pltpu.VMEM((2, 2, R, tile), F32), pltpu.VMEM((2, 2, R, piece), BF16), pltpu.VMEM((2, R, piece), BF16),
            dma((2,)), dma((2,)), dma((NQ,)), dma((NW, 2)), dma((2,)),
            dma((4,)), dma((2, 4)),
            dma((2,)), dma((2, 2)),
            dma((2,)), dma((2, 2)),
            dma((2, 2)), dma((2, 2)),
            dma((2, 2)), dma((2, 2)),
            dma((2, 2)), dma((2, 2)),
            dma((2, 2)), dma((2, 2)), dma((2, 2)), dma((2, 2)), dma,
        ]
        return pl.pallas_call(
            kernel,
            out_shape=jax.ShapeDtypeStruct((rows, width), BF16),
            in_specs=[hbm, vmem, hbm, hbm, hbm, hbm, hbm, hbm],
            out_specs=hbm,
            scratch_shapes=scratch,
            compiler_params=pltpu.CompilerParams(collective_id=0, has_side_effects=True, vmem_limit_bytes=67043328),
        )(x, gain.reshape(1, -1), jnp.asarray(cos), jnp.asarray(sin), wq, wk, wv, wo)

    tokens, columns = P("dp", None), P(None, "tp")
    return jax.shard_map(
        step,
        mesh=mesh,
        in_specs=(tokens, P(None), columns, columns, columns, P("tp", None)),
        out_specs=tokens,
        check_vma=False,
    )
```

```python
import functools

import jax
import jax.numpy as jnp
import numpy as np
from jax import lax
from jax.experimental import pallas as pl
from jax.experimental.pallas import tpu as pltpu
from jax.sharding import PartitionSpec as P

HEAD = 128
THETA = 10000
NEG = -1e30
HIDDEN = 2 * NEG
LOG2E = 1.4426950408889634
MESH = pl.DeviceIdType.MESH
F32, BF16 = jnp.float32, jnp.bfloat16

R = 256
WT = 512
NQ = 4
NW = 2
ORDER = ((1, 0), (1, 1), (1, 2), (0, 0), (1, 3), (0, 1), (0, 2), (0, 3))


def tables(rows):
    half = HEAD // 2
    rate = np.power(np.float32(THETA), -np.arange(half, dtype=np.float32) / np.float32(half)).astype(np.float32)
    angle = np.arange(rows, dtype=np.float32)[:, None] * rate
    cos, sin = np.cos(angle), np.sin(angle)
    return np.concatenate([cos, sin], 1).astype(np.float32)


def kernel(x_ref, gain_ref, table_ref, wq_ref, wk_ref, wv_ref, wo_ref, y_ref,
           gain_v, gain_s, xraw, xa, table_s, ring, wring, raw_s, qk_s, v_s, seen, top_s, mix_s,
           dsend, drecv, p1send, p1recv, p2send, p2recv, acc, fin, xres,
           x_sem, gain_sem, t_sem, ring_sem, wring_sem, xres_sem,
           d_ss, d_rs, p1_ss, p1_rs, p2_ss, p2_rs, p3_ss, p3_rs, p4_ss, p4_rs, p4f_ss, p4f_rs,
           loc_sem, e2_ss, e3_ss, e4_ss, e_rs):
    rows, width = x_ref.shape
    nc = rows // R
    heads = v_s.shape[0]
    cols = heads * HEAD
    half = width // 2
    tile = half // 4
    piece = tile // 2
    steps = cols // WT
    deep = width // 2
    quarter_rows = R // 4

    me = lax.axis_index("tp")
    core, yy, xx = lax.rem(me, 2), lax.rem(me // 2, 2), me // 4
    mate = me + 1 - 2 * core
    ypeer = me + 2 - 4 * yy
    xpeer = me + 4 - 8 * xx
    peers = (xpeer, ypeer)
    cross = (ypeer, xpeer)

    def remote(src, dst, ss, rs, to):
        return pltpu.make_async_remote_copy(src, dst, ss, rs, device_id={"tp": to}, device_id_type=MESH)

    def column(h, kind, s):
        a = kind % 2 == 0
        lead, other = (xx, yy) if a else (yy, xx)
        big = 1 - lead if kind < 2 else lead
        small = other if s == 0 else 1 - other
        return pl.multiple_of(h * half + (0 if a else 2 * tile) + big * tile + small * piece, piece)

    def at_rows(c):
        return pl.ds(pl.multiple_of(c * R, R), R)

    def x_copies(c):
        return [pltpu.make_async_copy(x_ref.at[pl.ds(pl.multiple_of(c * R + b * quarter_rows, quarter_rows), quarter_rows)],
                                      xraw.at[pl.ds(b * quarter_rows, quarter_rows)], x_sem.at[b]) for b in range(4)]

    def tile_copy(w, t, f):
        return pltpu.make_async_copy(w.at[pl.ds(f * deep, deep), pl.ds(pl.multiple_of(t * WT, WT), WT)], ring.at[2 * t + f], ring_sem.at[2 * t + f])

    def wo_copies(n, slot):
        mate_half, kind = ORDER[n]
        h = 1 - core if mate_half else core
        return [pltpu.make_async_copy(wo_ref.at[:, pl.ds(column(h, kind, s), piece)],
                                      wring.at[slot, :, pl.ds(s * piece, piece)], wring_sem.at[slot, s]) for s in range(2)]

    def d_copy(c, k):
        p = lax.rem(c, 2)
        return remote(dsend.at[k], drecv.at[p, k], d_ss.at[k], d_rs.at[p, k], mate)

    def p1_copy(c, k):
        p = lax.rem(c, 2)
        return remote(p1send.at[k], p1recv.at[k], p1_ss.at[k], p1_rs.at[p, k], peers[k])

    def p2_copy(c, k):
        p = lax.rem(c, 2)
        return remote(p2send.at[k], p2recv.at[p, k], p2_ss.at[k], p2_rs.at[p, k], cross[k])

    def mine(c, k):
        return y_ref.at[at_rows(c), pl.ds(column(core, 2 + k, 0), piece)]

    def p3_copy(c, k):
        p = lax.rem(c, 2)
        return remote(fin.at[p, k], mine(c, k), p3_ss.at[p, k], p3_rs.at[p, k], cross[k])

    def p4_copy(c, k):
        p = lax.rem(c, 2)
        return remote(fin.at[p, k], mine(c, k), p4_ss.at[p, k], p4_rs.at[p, k], peers[k])

    def e2_copy(c, k):
        p = lax.rem(c, 2)
        return remote(fin.at[p, k], mine(c, k), e2_ss.at[p, k], e_rs, mate)

    def loc_copy(c, k):
        p = lax.rem(c, 2)
        return pltpu.make_async_copy(fin.at[p, k], mine(c, k), loc_sem.at[p, k])

    def came3(c, k):
        return y_ref.at[at_rows(c), pl.ds(column(core, 2 + k, 1), piece)]

    def p4f_copy(c, k):
        p = lax.rem(c, 2)
        return remote(came3(c, k), came3(c, k), p4f_ss.at[p, k], p4f_rs.at[p, k], peers[k])

    def e3_copy(c, k):
        p = lax.rem(c, 2)
        return remote(came3(c, k), came3(c, k), e3_ss.at[p, k], e_rs, mate)

    def e4_copy(c, k):
        p = lax.rem(c, 2)
        lead = xx if k == 0 else yy
        first = pl.multiple_of(core * half + 2 * k * tile + (1 - lead) * tile, tile)
        there = y_ref.at[at_rows(c), pl.ds(first, tile)]
        return remote(there, there, e4_ss.at[p, k], e_rs, mate)

    def norm(first, count):
        lanes = [slice(n, n + HEAD) for n in range(0, width, HEAD)]
        for b in range(count):
            at = pl.ds(pl.multiple_of(first + b * 16, 16), 16)
            squares = [jnp.zeros((16, HEAD), F32)] * 4
            for n, lane in enumerate(lanes):
                wide = xraw[at, lane].astype(F32)
                squares[n % 4] += wide * wide
            total = jnp.sum(sum(squares[1:], squares[0]), -1, keepdims=True)
            scale = lax.rsqrt(total * (1 / width) + 1e-6)
            for lane in lanes:
                xa[at, lane] = (xraw[at, lane].astype(F32) * scale * gain_s[:, lane]).astype(BF16)

    gains = pltpu.make_async_copy(gain_ref, gain_v, gain_sem)
    gains.start()
    for copy in x_copies(0):
        copy.start()
    tile_copy(wq_ref, 0, 0).start()
    barrier = pltpu.get_barrier_semaphore()
    for to in (mate, xpeer, ypeer):
        pl.semaphore_signal(barrier, inc=1, device_id={"tp": to}, device_id_type=MESH)
    for t, f in ((0, 1), (1, 0), (1, 1)):
        tile_copy(wq_ref, t, f).start()
    turns = pltpu.make_async_copy(table_ref, table_s, t_sem)
    turns.start()
    gains.wait()
    gain_s[...] = jnp.broadcast_to(gain_v[...].astype(F32).reshape(1, width), gain_s.shape)

    def some(b, _):
        pltpu.make_async_copy(x_ref.at[pl.ds(0, quarter_rows)], xraw.at[pl.ds(b * quarter_rows, quarter_rows)], x_sem.at[b]).wait()
        norm(b * quarter_rows, quarter_rows // 16)
        return 0

    lax.fori_loop(0, 4, some, 0)
    for copy in x_copies(1):
        copy.start()
    for n in range(NW):
        for copy in wo_copies(n, n):
            copy.start()
    v_s[:, HEAD:, :] = jnp.ones((heads, 8, rows), BF16)
    turns.wait()

    def store_turned(i, j):
        here = at_rows(i)
        kind, t = j // steps, lax.rem(j, steps)
        both = table_s[here, :]
        other = pltpu.roll(both, HEAD // 2, 1)
        low = lax.broadcasted_iota(jnp.int32, both.shape, 1) < HEAD // 2
        cos, sin = jnp.where(low, both, other), jnp.where(low, -other, both)
        for n in range(WT // HEAD):
            h = t * (WT // HEAD) + n
            one_head = raw_s[:, n * HEAD:(n + 1) * HEAD].astype(F32)
            turned = (one_head * cos + pltpu.roll(one_head, HEAD // 2, 1) * sin).astype(BF16)
            to = kind * (h * rows + i * R) + (1 - kind) * (heads * rows + h * R)
            qk_s[pl.ds(pl.multiple_of(to, R), R), :] = turned

    def store_values(i, t):
        for n in range(WT // HEAD):
            v_s[t * (WT // HEAD) + n, pl.ds(0, HEAD), at_rows(i)] = raw_s[:, n * HEAD:(n + 1) * HEAD].T

    def step(t, store, follow):
        out = None
        for f in range(2):
            pltpu.make_async_copy(wq_ref.at[pl.ds(0, deep), pl.ds(0, WT)], ring.at[2 * t + f], ring_sem.at[2 * t + f]).wait()
            if f == 0:
                store()
                out = jnp.dot(xa[:, :deep], ring[2 * t], preferred_element_type=F32)
            else:
                raw_s[...] = (out + jnp.dot(xa[:, deep:], ring[2 * t + 1], preferred_element_type=F32)).astype(BF16)
            follow(f)

    def queries_keys(i):
        def one(j, _):
            t = lax.rem(j, steps)

            def follow(f):
                for n, w in enumerate((wk_ref, wv_ref)):
                    @pl.when(j // steps == n)
                    def _():
                        tile_copy(w, t, f).start()

            step(t, lambda: store_turned(i, jnp.maximum(j - 1, 0)), follow)
            return 0

        lax.fori_loop(0, 2 * steps, one, 0)

    def values(i):
        for t in range(steps):
            def follow(f):
                @pl.when(i + 1 < nc)
                def _():
                    tile_copy(wq_ref, t, f).start()

            step(t, (lambda: store_turned(i, 2 * steps - 1)) if t == 0 else (lambda: store_values(i, t - 1)), follow)
        store_values(i, steps - 1)

    def attention(i):
        e = HEAD**-0.5 * LOG2E
        for h in range(heads):
            top_s[h:h + 1, :] = jnp.full((1, R), NEG, F32)
            mix_s[h] = jnp.zeros((HEAD + 8, R), F32)

        def block(j, nk, masked):
            here = pl.ds(pl.multiple_of(j * R, R), nk * R)

            def score(h):
                keys = qk_s[pl.ds(pl.multiple_of(h * rows + j * R, R), nk * R), :]
                queries = qk_s[heads * rows + h * R:heads * rows + (h + 1) * R, :]
                return lax.dot_general(keys, queries, (((1,), (1,)), ((), ())), preferred_element_type=F32)

            def mix(h, weight, keep):
                mix_s[h] = mix_s[h] * keep + jnp.dot(v_s[h, :, here], weight, preferred_element_type=F32)

            if masked:
                ok = lax.broadcasted_iota(jnp.int32, (nk * R, R), 1) + (nk - 1) * R >= lax.broadcasted_iota(jnp.int32, (nk * R, R), 0)
            def soft(h, s):
                if masked:
                    s = jnp.where(ok, s, HIDDEN)
                old = top_s[h:h + 1, :]
                top = jnp.maximum(old, s.max(axis=0, keepdims=True))
                top_s[h:h + 1, :] = top
                return jnp.exp2((s - top) * e).astype(BF16), jnp.exp2((old - top) * e)
            scores = [score(h) for h in range(heads)]
            ws = [soft(h, scores[h]) for h in range(heads)]
            for h in range(heads):
                mix(h, *ws[h])

        def whole(j, _):
            block(j * 2, 2, False)
            return 0

        lax.fori_loop(0, i // 2, whole, 0)

        @pl.when(lax.rem(i, 2) == 0)
        def _():
            block(i, 1, True)

        @pl.when(lax.rem(i, 2) == 1)
        def _():
            block(i - 1, 2, True)

        for h in range(heads):
            total = mix_s[h, HEAD:HEAD + 1, :]
            seen[:, h * HEAD:(h + 1) * HEAD] = (mix_s[h, :HEAD, :] * (1 / total)).T.astype(BF16)

    def output(i):
        p = lax.rem(i, 2)

        @pl.when(i + 1 < nc)
        def _():
            for copy in x_copies(i + 1):
                copy.wait()

        for n, (mate_half, k) in enumerate(ORDER):
            slot = lax.rem(i * 8 + n, NW)
            for copy in wo_copies(n, slot):
                copy.wait()
            if not mate_half:
                d_copy(i, k).wait_recv()
            norm(n * (R // 8), R // 8 // 16)
            out = jnp.dot(seen[...], wring[slot], preferred_element_type=F32)
            if mate_half:
                dsend[k] = out.astype(BF16)
            elif k < 2:
                p1send[k] = (out + drecv[p, k].astype(F32)).astype(BF16)
            else:
                acc[k - 2] = out + drecv[p, k].astype(F32)
            after = n + NW
            if after < 8:
                for copy in wo_copies(after, slot):
                    copy.start()
            else:
                @pl.when(i + 1 < nc)
                def _():
                    for copy in wo_copies(after - 8, slot):
                        copy.start()
            if mate_half:
                d_copy(i, k).start()
            elif k < 2:
                p1_copy(i, k).start()

        @pl.when(i + 2 < nc)
        def _():
            for copy in x_copies(i + 2):
                copy.start()

    def xres_copy(c, k):
        return pltpu.make_async_copy(x_ref.at[at_rows(c), pl.ds(column(core, 2 + k, 0), piece)], xres.at[k], xres_sem.at[k])

    def second(c):
        p = lax.rem(c, 2)
        for k in range(4):
            d_copy(c, k).wait_send()
        for k in range(2):
            p1_copy(c, k).wait()
            xres_copy(c, k).start()

            @pl.when(c > 0)
            def _():
                p2_copy(c - 1, k).wait_send()
        for k in range(2):
            p2send[k] = (acc[k, :, piece:] + p1recv[k, :, piece:].astype(F32)).astype(BF16)
            acc[k, :, :piece] = acc[k, :, :piece] + p1recv[k, :, :piece].astype(F32)
        for k in range(2):
            p2_copy(c, k).start()

    def third(c):
        p = lax.rem(c, 2)

        @pl.when(c >= 2)
        def _():
            done_fin(c - 2)

        for k in range(2):
            p2_copy(c, k).wait_recv()
            xres_copy(c, k).wait()
        for k in range(2):
            fin[p, k] = (acc[k, :, :piece] + p2recv[p, k].astype(F32) + xres[k].astype(F32)).astype(BF16)
        for k in range(2):
            p3_copy(c, k).start()
        for k in range(2):
            loc_copy(c, k).start()
            e2_copy(c, k).start()

    def done_fin(c):
        for k in range(2):
            p3_copy(c, k).wait_send()
            p4_copy(c, k).wait_send()
            e2_copy(c, k).wait_send()
            loc_copy(c, k).wait()

    def done_fwd(c):
        for k in range(2):
            p4f_copy(c, k).wait_send()
            e3_copy(c, k).wait_send()

    def forward(c):
        @pl.when(c >= 2)
        def _():
            done_fwd(c - 2)

        for k in range(2):
            p3_copy(c, k).wait_recv()
            p4f_copy(c, k).start()
        for k in range(2):
            e3_copy(c, k).start()

    def last(c):
        @pl.when(c >= 2)
        def _():
            for k in range(2):
                e4_copy(c - 2, k).wait_send()

        for k in range(2):
            p4_copy(c, k).wait_recv()
            p4f_copy(c, k).wait_recv()
            e4_copy(c, k).start()

    def iteration(i, _):
        @pl.when(i < nc)
        def _():
            queries_keys(i)

        @pl.when(i == 0)
        def _():
            pl.semaphore_wait(barrier, 3)

        @pl.when((i >= 1) & (i < nc + 1))
        def _():
            second(i - 1)

        @pl.when((i >= 2) & (i < nc + 2))
        def _():
            forward(i - 2)

        @pl.when(i < nc)
        def _():
            values(i)
            attention(i)

        @pl.when((i >= 1) & (i < nc + 1))
        def _():
            third(i - 1)

        @pl.when(i < nc)
        def _():
            output(i)

        @pl.when((i >= 1) & (i < nc + 1))
        def _():
            for k in range(2):
                p4_copy(i - 1, k).start()

        @pl.when(i >= 2)
        def _():
            last(i - 2)

        return 0

    lax.fori_loop(0, nc + 2, iteration, 0)

    for k in range(2):
        p2_copy(nc - 1, k).wait_send()
    for c in (nc - 2, nc - 1):
        done_fin(c)
        done_fwd(c)
        for k in range(2):
            e4_copy(c, k).wait_send()
    theirs = y_ref.at[:, pl.ds(pl.multiple_of((1 - core) * half, half), half)]
    remote(theirs, theirs, e2_ss.at[0, 0], e_rs, mate).wait_recv()


def solution(mesh):
    def step(x, gain, wq, wk, wv, wo):
        rows, width = x.shape
        cols = wq.shape[1]
        heads = cols // HEAD
        half, tile, piece = width // 2, width // 8, width // 16
        hbm = pl.BlockSpec(memory_space=pl.ANY)
        dma = pltpu.SemaphoreType.DMA
        scratch = [
            pltpu.VMEM((width,), BF16), pltpu.VMEM((16, width), F32),
            pltpu.VMEM((R, width), BF16), pltpu.VMEM((R, width), BF16),
            pltpu.VMEM((rows, HEAD), F32),
            pltpu.VMEM((NQ, width // 2, WT), BF16), pltpu.VMEM((NW, cols, tile), BF16),
            pltpu.VMEM((R, WT), BF16), pltpu.VMEM((heads * (rows + R), HEAD), BF16), pltpu.VMEM((heads, HEAD + 8, rows), BF16),
            pltpu.VMEM((R, cols), BF16), pltpu.VMEM((heads, R), F32), pltpu.VMEM((heads, HEAD + 8, R), F32),
            pltpu.VMEM((4, R, tile), BF16), pltpu.VMEM((2, 4, R, tile), BF16),
            pltpu.VMEM((2, R, tile), BF16), pltpu.VMEM((2, R, tile), BF16),
            pltpu.VMEM((2, R, piece), BF16), pltpu.VMEM((2, 2, R, piece), BF16),
            pltpu.VMEM((2, R, tile), F32), pltpu.VMEM((2, 2, R, piece), BF16), pltpu.VMEM((2, R, piece), BF16),
            dma((4,)), dma, dma, dma((NQ,)), dma((NW, 2)), dma((2,)),
            dma((4,)), dma((2, 4)),
            dma((2,)), dma((2, 2)),
            dma((2,)), dma((2, 2)),
            dma((2, 2)), dma((2, 2)),
            dma((2, 2)), dma((2, 2)),
            dma((2, 2)), dma((2, 2)),
            dma((2, 2)), dma((2, 2)), dma((2, 2)), dma((2, 2)), dma,
        ]
        return pl.pallas_call(
            kernel,
            out_shape=jax.ShapeDtypeStruct((rows, width), BF16),
            in_specs=[hbm] * 7,
            out_specs=hbm,
            scratch_shapes=scratch,
            compiler_params=pltpu.CompilerParams(collective_id=0, has_side_effects=True, vmem_limit_bytes=67043328),
        )(x, gain, jnp.asarray(tables(rows)), wq, wk, wv, wo)

    tokens, columns = P("dp", None), P(None, "tp")
    return jax.shard_map(
        step,
        mesh=mesh,
        in_specs=(tokens, P(None), columns, columns, columns, P("tp", None)),
        out_specs=tokens,
        check_vma=False,
    )
```

```python
import functools

import jax
import jax.numpy as jnp
import numpy as np
from jax import lax
from jax.experimental import pallas as pl
from jax.experimental.pallas import tpu as pltpu
from jax.sharding import PartitionSpec as P

HEAD = 128
THETA = 10000
NEG = -1e30
HIDDEN = 2 * NEG
LOG2E = 1.4426950408889634
MESH = pl.DeviceIdType.MESH
F32, BF16 = jnp.float32, jnp.bfloat16

R = 256
WT = 512
NQ = 4
NW = 2
ORDER = ((1, 0), (1, 1), (1, 2), (0, 0), (1, 3), (0, 1), (0, 2), (0, 3))


def tables(rows):
    half = HEAD // 2
    rate = np.power(np.float32(THETA), -np.arange(half, dtype=np.float32) / np.float32(half)).astype(np.float32)
    angle = np.arange(rows, dtype=np.float32)[:, None] * rate
    cos, sin = np.cos(angle), np.sin(angle)
    return np.concatenate([cos, sin], 1).astype(np.float32)


def kernel(x_ref, gain_ref, table_ref, wq_ref, wk_ref, wv_ref, wo_ref, y_ref, own_ref,
           gain_v, gain_s, xraw, xa, table_s, ring, wring, raw_s, qk_s, v_s, seen, top_s, mix_s,
           dsend, drecv, p1send, p1recv, p2send, p2recv, acc, fin, xres,
           x_sem, gain_sem, t_sem, ring_sem, wring_sem, xres_sem,
           d_ss, d_rs, p1_ss, p1_rs, p2_ss, p2_rs, p3_ss, p3_rs, p4_ss, p4_rs, p4f_ss, p4f_rs,
           loc_sem, e2_ss, e3_ss, e4_ss, e_rs):
    rows, width = x_ref.shape
    nc = rows // R
    heads = v_s.shape[0]
    cols = heads * HEAD
    half = width // 2
    tile = half // 4
    piece = tile // 2
    steps = cols // WT
    deep = width // 2
    quarter_rows = R // 4

    me = lax.axis_index("tp")
    core, yy, xx = lax.rem(me, 2), lax.rem(me // 2, 2), me // 4
    mate = me + 1 - 2 * core
    ypeer = me + 2 - 4 * yy
    xpeer = me + 4 - 8 * xx
    peers = (xpeer, ypeer)
    cross = (ypeer, xpeer)

    def remote(src, dst, ss, rs, to):
        return pltpu.make_async_remote_copy(src, dst, ss, rs, device_id={"tp": to}, device_id_type=MESH)

    def column(h, kind, s):
        a = kind % 2 == 0
        lead, other = (xx, yy) if a else (yy, xx)
        big = 1 - lead if kind < 2 else lead
        small = other if s == 0 else 1 - other
        return pl.multiple_of(h * half + (0 if a else 2 * tile) + big * tile + small * piece, piece)

    def at_rows(c):
        return pl.ds(pl.multiple_of(c * R, R), R)

    def x_copies(c):
        return [pltpu.make_async_copy(x_ref.at[pl.ds(pl.multiple_of(c * R + b * quarter_rows, quarter_rows), quarter_rows)],
                                      xraw.at[pl.ds(b * quarter_rows, quarter_rows)], x_sem.at[b]) for b in range(4)]

    def tile_copy(w, t, f):
        return pltpu.make_async_copy(w.at[pl.ds(f * deep, deep), pl.ds(pl.multiple_of(t * WT, WT), WT)], ring.at[2 * t + f], ring_sem.at[2 * t + f])

    def wo_copies(n, slot):
        mate_half, kind = ORDER[n]
        h = 1 - core if mate_half else core
        return [pltpu.make_async_copy(wo_ref.at[:, pl.ds(column(h, kind, s), piece)],
                                      wring.at[slot, :, pl.ds(s * piece, piece)], wring_sem.at[slot, s]) for s in range(2)]

    def d_copy(c, k):
        p = lax.rem(c, 2)
        return remote(dsend.at[k], drecv.at[p, k], d_ss.at[k], d_rs.at[p, k], mate)

    def p1_copy(c, k):
        p = lax.rem(c, 2)
        return remote(p1send.at[k], p1recv.at[k], p1_ss.at[k], p1_rs.at[p, k], peers[k])

    def p2_copy(c, k):
        p = lax.rem(c, 2)
        return remote(p2send.at[k], p2recv.at[p, k], p2_ss.at[k], p2_rs.at[p, k], cross[k])

    def mine(c, k):
        return y_ref.at[at_rows(c), pl.ds(column(core, 2 + k, 0), piece)]

    def p3_copy(c, k):
        p = lax.rem(c, 2)
        return remote(fin.at[p, k], mine(c, k), p3_ss.at[p, k], p3_rs.at[p, k], cross[k])

    def p4_copy(c, k):
        p = lax.rem(c, 2)
        return remote(fin.at[p, k], mine(c, k), p4_ss.at[p, k], p4_rs.at[p, k], peers[k])

    def e2_copy(c, k):
        p = lax.rem(c, 2)
        return remote(fin.at[p, k], mine(c, k), e2_ss.at[p, k], e_rs, mate)

    def loc_copy(c, k):
        p = lax.rem(c, 2)
        return pltpu.make_async_copy(fin.at[p, k], mine(c, k), loc_sem.at[p, k])

    def own_copy(k):
        p = (nc - 1) % 2
        return pltpu.make_async_copy(fin.at[p, k], own_ref.at[k], loc_sem.at[p, k])

    def came3(c, k):
        return y_ref.at[at_rows(c), pl.ds(column(core, 2 + k, 1), piece)]

    def p4f_copy(c, k):
        p = lax.rem(c, 2)
        return remote(came3(c, k), came3(c, k), p4f_ss.at[p, k], p4f_rs.at[p, k], peers[k])

    def e3_copy(c, k):
        p = lax.rem(c, 2)
        return remote(came3(c, k), came3(c, k), e3_ss.at[p, k], e_rs, mate)

    def e4_copy(c, k):
        p = lax.rem(c, 2)
        lead = xx if k == 0 else yy
        first = pl.multiple_of(core * half + 2 * k * tile + (1 - lead) * tile, tile)
        there = y_ref.at[at_rows(c), pl.ds(first, tile)]
        return remote(there, there, e4_ss.at[p, k], e_rs, mate)

    def norm(first, count):
        lanes = [slice(n, n + HEAD) for n in range(0, width, HEAD)]
        for b in range(count):
            at = pl.ds(pl.multiple_of(first + b * 16, 16), 16)
            squares = [jnp.zeros((16, HEAD), F32)] * 4
            for n, lane in enumerate(lanes):
                wide = xraw[at, lane].astype(F32)
                squares[n % 4] += wide * wide
            total = jnp.sum(sum(squares[1:], squares[0]), -1, keepdims=True)
            scale = lax.rsqrt(total * (1 / width) + 1e-6)
            for lane in lanes:
                xa[at, lane] = (xraw[at, lane].astype(F32) * scale * gain_s[:, lane]).astype(BF16)

    gains = pltpu.make_async_copy(gain_ref, gain_v, gain_sem)
    gains.start()
    for copy in x_copies(0):
        copy.start()
    tile_copy(wq_ref, 0, 0).start()
    barrier = pltpu.get_barrier_semaphore()
    for to in (mate, xpeer, ypeer):
        pl.semaphore_signal(barrier, inc=1, device_id={"tp": to}, device_id_type=MESH)
    for t, f in ((0, 1), (1, 0), (1, 1)):
        tile_copy(wq_ref, t, f).start()
    turns = pltpu.make_async_copy(table_ref, table_s, t_sem)
    turns.start()
    gains.wait()
    gain_s[...] = jnp.broadcast_to(gain_v[...].astype(F32).reshape(1, width), gain_s.shape)

    def some(b, _):
        pltpu.make_async_copy(x_ref.at[pl.ds(0, quarter_rows)], xraw.at[pl.ds(b * quarter_rows, quarter_rows)], x_sem.at[b]).wait()
        norm(b * quarter_rows, quarter_rows // 16)
        return 0

    lax.fori_loop(0, 4, some, 0)
    for copy in x_copies(1):
        copy.start()
    for n in range(NW):
        for copy in wo_copies(n, n):
            copy.start()
    v_s[:, HEAD:, :] = jnp.ones((heads, 8, rows), BF16)
    turns.wait()

    def store_turned(i, j):
        here = at_rows(i)
        kind, t = j // steps, lax.rem(j, steps)
        both = table_s[here, :]
        other = pltpu.roll(both, HEAD // 2, 1)
        low = lax.broadcasted_iota(jnp.int32, both.shape, 1) < HEAD // 2
        cos, sin = jnp.where(low, both, other), jnp.where(low, -other, both)
        for n in range(WT // HEAD):
            h = t * (WT // HEAD) + n
            one_head = raw_s[:, n * HEAD:(n + 1) * HEAD].astype(F32)
            turned = (one_head * cos + pltpu.roll(one_head, HEAD // 2, 1) * sin).astype(BF16)
            to = kind * (h * rows + i * R) + (1 - kind) * (heads * rows + h * R)
            qk_s[pl.ds(pl.multiple_of(to, R), R), :] = turned

    def store_values(i, t):
        for n in range(WT // HEAD):
            v_s[t * (WT // HEAD) + n, pl.ds(0, HEAD), at_rows(i)] = raw_s[:, n * HEAD:(n + 1) * HEAD].T

    def step(t, store, follow):
        out = None
        for f in range(2):
            pltpu.make_async_copy(wq_ref.at[pl.ds(0, deep), pl.ds(0, WT)], ring.at[2 * t + f], ring_sem.at[2 * t + f]).wait()
            if f == 0:
                store()
                out = jnp.dot(xa[:, :deep], ring[2 * t], preferred_element_type=F32)
            else:
                raw_s[...] = (out + jnp.dot(xa[:, deep:], ring[2 * t + 1], preferred_element_type=F32)).astype(BF16)
            follow(f)

    def queries_keys(i):
        def one(j, _):
            t = lax.rem(j, steps)

            def follow(f):
                for n, w in enumerate((wk_ref, wv_ref)):
                    @pl.when(j // steps == n)
                    def _():
                        tile_copy(w, t, f).start()

            step(t, lambda: store_turned(i, jnp.maximum(j - 1, 0)), follow)
            return 0

        lax.fori_loop(0, 2 * steps, one, 0)

    def values(i):
        for t in range(steps):
            def follow(f):
                @pl.when(i + 1 < nc)
                def _():
                    tile_copy(wq_ref, t, f).start()

            step(t, (lambda: store_turned(i, 2 * steps - 1)) if t == 0 else (lambda: store_values(i, t - 1)), follow)
        store_values(i, steps - 1)

    def attention(i):
        e = HEAD**-0.5 * LOG2E
        for h in range(heads):
            top_s[h:h + 1, :] = jnp.full((1, R), NEG, F32)
            mix_s[h] = jnp.zeros((HEAD + 8, R), F32)

        def block(j, nk, masked):
            here = pl.ds(pl.multiple_of(j * R, R), nk * R)

            def score(h):
                keys = qk_s[pl.ds(pl.multiple_of(h * rows + j * R, R), nk * R), :]
                queries = qk_s[heads * rows + h * R:heads * rows + (h + 1) * R, :]
                return lax.dot_general(keys, queries, (((1,), (1,)), ((), ())), preferred_element_type=F32)

            def mix(h, weight, keep):
                mix_s[h] = mix_s[h] * keep + jnp.dot(v_s[h, :, here], weight, preferred_element_type=F32)

            if masked:
                ok = lax.broadcasted_iota(jnp.int32, (nk * R, R), 1) + (nk - 1) * R >= lax.broadcasted_iota(jnp.int32, (nk * R, R), 0)
            def soft(h, s):
                if masked:
                    s = jnp.where(ok, s, HIDDEN)
                old = top_s[h:h + 1, :]
                top = jnp.maximum(old, s.max(axis=0, keepdims=True))
                top_s[h:h + 1, :] = top
                return jnp.exp2((s - top) * e).astype(BF16), jnp.exp2((old - top) * e)
            scores = [score(h) for h in range(heads)]
            ws = [soft(h, scores[h]) for h in range(heads)]
            for h in range(heads):
                mix(h, *ws[h])

        def whole(j, _):
            block(j * 2, 2, False)
            return 0

        lax.fori_loop(0, i // 2, whole, 0)

        @pl.when(lax.rem(i, 2) == 0)
        def _():
            block(i, 1, True)

        @pl.when(lax.rem(i, 2) == 1)
        def _():
            block(i - 1, 2, True)

        for h in range(heads):
            total = mix_s[h, HEAD:HEAD + 1, :]
            seen[:, h * HEAD:(h + 1) * HEAD] = (mix_s[h, :HEAD, :] * (1 / total)).T.astype(BF16)

    def output(i):
        p = lax.rem(i, 2)

        @pl.when(i + 1 < nc)
        def _():
            for copy in x_copies(i + 1):
                copy.wait()

        for n, (mate_half, k) in enumerate(ORDER):
            slot = lax.rem(i * 8 + n, NW)
            for copy in wo_copies(n, slot):
                copy.wait()
            if not mate_half:
                d_copy(i, k).wait_recv()
            norm(n * (R // 8), R // 8 // 16)
            out = jnp.dot(seen[...], wring[slot], preferred_element_type=F32)
            if mate_half:
                dsend[k] = out.astype(BF16)
            elif k < 2:
                p1send[k] = (out + drecv[p, k].astype(F32)).astype(BF16)
            else:
                acc[k - 2] = out + drecv[p, k].astype(F32)
            after = n + NW
            if after < 8:
                for copy in wo_copies(after, slot):
                    copy.start()
            else:
                @pl.when(i + 1 < nc)
                def _():
                    for copy in wo_copies(after - 8, slot):
                        copy.start()
            if mate_half:
                d_copy(i, k).start()
            elif k < 2:
                p1_copy(i, k).start()

        @pl.when(i + 2 < nc)
        def _():
            for copy in x_copies(i + 2):
                copy.start()

    def xres_copy(c, k):
        return pltpu.make_async_copy(x_ref.at[at_rows(c), pl.ds(column(core, 2 + k, 0), piece)], xres.at[k], xres_sem.at[k])

    def second(c):
        p = lax.rem(c, 2)
        for k in range(4):
            d_copy(c, k).wait_send()
        for k in range(2):
            p1_copy(c, k).wait()
            xres_copy(c, k).start()

            @pl.when(c > 0)
            def _():
                p2_copy(c - 1, k).wait_send()
        for k in range(2):
            p2send[k] = (acc[k, :, piece:] + p1recv[k, :, piece:].astype(F32)).astype(BF16)
            acc[k, :, :piece] = acc[k, :, :piece] + p1recv[k, :, :piece].astype(F32)
        for k in range(2):
            p2_copy(c, k).start()

    def third(c):
        p = lax.rem(c, 2)

        @pl.when(c >= 2)
        def _():
            done_fin(c - 2)

        for k in range(2):
            p2_copy(c, k).wait_recv()
            xres_copy(c, k).wait()
        for k in range(2):
            fin[p, k] = (acc[k, :, :piece] + p2recv[p, k].astype(F32) + xres[k].astype(F32)).astype(BF16)

        @pl.when(c < nc - 1)
        def _():
            for k in range(2):
                p3_copy(c, k).start()
            for k in range(2):
                loc_copy(c, k).start()
                e2_copy(c, k).start()

        @pl.when(c == nc - 1)
        def _():
            for k in range(2):
                own_copy(k).start()

    def done_fin(c):
        for k in range(2):
            p3_copy(c, k).wait_send()
            p4_copy(c, k).wait_send()
            e2_copy(c, k).wait_send()
            loc_copy(c, k).wait()

    def done_fwd(c):
        for k in range(2):
            p4f_copy(c, k).wait_send()
            e3_copy(c, k).wait_send()

    def forward(c):
        @pl.when(c >= 2)
        def _():
            done_fwd(c - 2)

        for k in range(2):
            p3_copy(c, k).wait_recv()
            p4f_copy(c, k).start()
        for k in range(2):
            e3_copy(c, k).start()

    def last(c):
        @pl.when(c >= 2)
        def _():
            for k in range(2):
                e4_copy(c - 2, k).wait_send()

        for k in range(2):
            p4_copy(c, k).wait_recv()
            p4f_copy(c, k).wait_recv()
            e4_copy(c, k).start()

    def iteration(i, _):
        @pl.when(i < nc)
        def _():
            queries_keys(i)

        @pl.when(i == 0)
        def _():
            pl.semaphore_wait(barrier, 3)

        @pl.when(i == nc)
        def _():
            forward(nc - 2)

        @pl.when(i >= 1)
        def _():
            second(i - 1)

        @pl.when((i >= 2) & (i < nc))
        def _():
            forward(i - 2)

        @pl.when(i < nc)
        def _():
            values(i)
            attention(i)

        @pl.when(i == nc)
        def _():
            last(nc - 2)

        @pl.when(i >= 1)
        def _():
            third(i - 1)

        @pl.when(i < nc)
        def _():
            output(i)

        @pl.when((i >= 1) & (i < nc))
        def _():
            for k in range(2):
                p4_copy(i - 1, k).start()

        @pl.when((i >= 2) & (i < nc))
        def _():
            last(i - 2)

        return 0

    lax.fori_loop(0, nc + 1, iteration, 0)

    done_fin(nc - 2)
    for k in range(2):
        p2_copy(nc - 1, k).wait_send()
        own_copy(k).wait()
    for c in (nc - 3, nc - 2):
        done_fwd(c)
        for k in range(2):
            e4_copy(c, k).wait_send()
    theirs = y_ref.at[pl.ds(0, (nc - 1) * R), pl.ds(pl.multiple_of((1 - core) * half, half), half)]
    remote(theirs, theirs, e2_ss.at[0, 0], e_rs, mate).wait_recv()


FIRST = 1152
SLOTS, AHEAD, STRIP = 8, 4, 128


def moved(y, into, first, count):
    width = y.shape[1]
    n = count // STRIP

    def body(*refs):
        src, dst, buf, in_sem, out_sem = refs[0], *refs[-4:]

        def rows_of(j):
            return pl.ds(pl.multiple_of(first + j * STRIP, STRIP), STRIP)

        def read(j):
            slot = lax.rem(j, SLOTS)
            return pltpu.make_async_copy(src.at[rows_of(j)], buf.at[slot], in_sem.at[slot])

        def write(j):
            slot = lax.rem(j, SLOTS)
            return pltpu.make_async_copy(buf.at[slot], dst.at[rows_of(j)], out_sem.at[slot])

        for j in range(min(AHEAD, n)):
            read(jnp.int32(j)).start()

        def one(j, _):
            read(j).wait()
            write(j).start()

            @pl.when((j + AHEAD < n) & (j + AHEAD >= SLOTS))
            def _():
                write(j + AHEAD - SLOTS).wait()

            @pl.when(j + AHEAD < n)
            def _():
                read(j + AHEAD).start()
            return 0

        lax.fori_loop(0, n, one, 0)
        for j in range(max(n - SLOTS, 0), n):
            write(jnp.int32(j)).wait()

    given = (y,) if into is None else (y, into)
    return pl.pallas_call(
        body,
        out_shape=jax.ShapeDtypeStruct(y.shape, y.dtype),
        in_specs=[pl.BlockSpec(memory_space=pl.ANY)] * len(given),
        out_specs=pl.BlockSpec(memory_space=pl.ANY),
        scratch_shapes=[pltpu.VMEM((SLOTS, STRIP, width), BF16), pltpu.SemaphoreType.DMA((SLOTS,)), pltpu.SemaphoreType.DMA((SLOTS,))],
        input_output_aliases={} if into is None else {1: 0},
        cost_estimate=pl.CostEstimate(flops=0, transcendentals=0, bytes_accessed=4 * count * width),
        name="moved%d" % first,
    )(*given)


def placed(y, halves):
    rows, width = y.shape
    piece, tile, half = width // 16, width // 8, width // 2

    def body(*refs):
        dst, buf, in_sem, out_sem = refs[-4:]
        me = lax.axis_index("tp")
        core, yy, xx = lax.rem(me, 2), lax.rem(me // 2, 2), me // 4
        reads, writes = [], []
        for n in range(2):
            own, from_y, from_x, far_a, far_b = refs[1 + 5 * n:6 + 5 * n]
            base = (core if n == 0 else 1 - core) * half
            for src, b, big, small in ((own.at[0], 0, xx, yy), (from_y.at[0], 0, xx, 1 - yy), (from_x.at[0], 0, 1 - xx, yy),
                                       (far_a, 0, 1 - xx, 1 - yy), (own.at[1], 1, yy, xx), (from_x.at[1], 1, yy, 1 - xx),
                                       (from_y.at[1], 1, 1 - yy, xx), (far_b, 1, 1 - yy, 1 - xx)):
                at = len(reads)
                to = pl.multiple_of(base + 2 * b * tile + big * tile + small * piece, piece)
                reads.append(pltpu.make_async_copy(src, buf.at[at], in_sem.at[at]))
                writes.append(pltpu.make_async_copy(buf.at[at], dst.at[pl.ds(rows - R, R), pl.ds(to, piece)], out_sem.at[at]))
        for copy in reads:
            copy.start()
        for read, write in zip(reads, writes):
            read.wait()
            write.start()
        for copy in writes:
            copy.wait()

    given = (y, *halves[0], *halves[1])
    return pl.pallas_call(
        body,
        out_shape=jax.ShapeDtypeStruct(y.shape, y.dtype),
        in_specs=[pl.BlockSpec(memory_space=pl.ANY)] * len(given),
        out_specs=pl.BlockSpec(memory_space=pl.ANY),
        scratch_shapes=[pltpu.VMEM((16, R, piece), BF16), pltpu.SemaphoreType.DMA((16,)), pltpu.SemaphoreType.DMA((16,))],
        input_output_aliases={0: 0},
        cost_estimate=pl.CostEstimate(flops=0, transcendentals=0, bytes_accessed=4 * R * width),
    )(*given)


def solution(mesh):
    def step(x, gain, wq, wk, wv, wo):
        rows, width = x.shape
        cols = wq.shape[1]
        heads = cols // HEAD
        half, tile, piece = width // 2, width // 8, width // 16
        hbm = pl.BlockSpec(memory_space=pl.ANY)
        dma = pltpu.SemaphoreType.DMA
        scratch = [
            pltpu.VMEM((width,), BF16), pltpu.VMEM((16, width), F32),
            pltpu.VMEM((R, width), BF16), pltpu.VMEM((R, width), BF16),
            pltpu.VMEM((rows, HEAD), F32),
            pltpu.VMEM((NQ, width // 2, WT), BF16), pltpu.VMEM((NW, cols, tile), BF16),
            pltpu.VMEM((R, WT), BF16), pltpu.VMEM((heads * (rows + R), HEAD), BF16), pltpu.VMEM((heads, HEAD + 8, rows), BF16),
            pltpu.VMEM((R, cols), BF16), pltpu.VMEM((heads, R), F32), pltpu.VMEM((heads, HEAD + 8, R), F32),
            pltpu.VMEM((4, R, tile), BF16), pltpu.VMEM((2, 4, R, tile), BF16),
            pltpu.VMEM((2, R, tile), BF16), pltpu.VMEM((2, R, tile), BF16),
            pltpu.VMEM((2, R, piece), BF16), pltpu.VMEM((2, 2, R, piece), BF16),
            pltpu.VMEM((2, R, tile), F32), pltpu.VMEM((2, 2, R, piece), BF16), pltpu.VMEM((2, R, piece), BF16),
            dma((4,)), dma, dma, dma((NQ,)), dma((NW, 2)), dma((2,)),
            dma((4,)), dma((2, 4)),
            dma((2,)), dma((2, 2)),
            dma((2,)), dma((2, 2)),
            dma((2, 2)), dma((2, 2)),
            dma((2, 2)), dma((2, 2)),
            dma((2, 2)), dma((2, 2)),
            dma((2, 2)), dma((2, 2)), dma((2, 2)), dma((2, 2)), dma,
        ]
        most, own = pl.pallas_call(
            kernel,
            out_shape=[jax.ShapeDtypeStruct((rows, width), BF16), jax.ShapeDtypeStruct((2, R, piece), BF16)],
            in_specs=[hbm] * 7,
            out_specs=[hbm, hbm],
            scratch_shapes=scratch,
            compiler_params=pltpu.CompilerParams(collective_id=0, has_side_effects=True, vmem_limit_bytes=67043328),
        )(x, gain, jnp.asarray(tables(rows)), wq, wk, wv, wo)

        def sent(t, bit):
            return lax.ppermute(t, "tp", [(d, d ^ bit) for d in range(8)])

        to_mate, to_y, to_x = 1, 2, 4
        from_y, from_x = sent(own, to_y), sent(own, to_x)
        mates = [sent(own, to_mate)]
        y = moved(most, None, 0, FIRST)
        y, from_y, from_x = lax.optimization_barrier((y, from_y, from_x))
        far = [sent(from_y[0], to_x), sent(from_x[1], to_y)]
        mates += [sent(from_y, to_mate), sent(from_x, to_mate)]
        y = moved(most, y, FIRST, rows - R - FIRST)
        y, *far = lax.optimization_barrier((y, *far))
        mates += [sent(t, to_mate) for t in far]
        return placed(y, ([own, from_y, from_x, *far], mates))

    tokens, columns = P("dp", None), P(None, "tp")
    return jax.shard_map(
        step,
        mesh=mesh,
        in_specs=(tokens, P(None), columns, columns, columns, P("tp", None)),
        out_specs=tokens,
        check_vma=False,
    )
```

```python
import functools

import jax
import jax.numpy as jnp
import numpy as np
from jax import lax
from jax.experimental import pallas as pl
from jax.experimental.pallas import tpu as pltpu
from jax.sharding import PartitionSpec as P

HEAD = 128
THETA = 10000
NEG = -1e30
HIDDEN = 2 * NEG
LOG2E = 1.4426950408889634
MESH = pl.DeviceIdType.MESH
F32, BF16 = jnp.float32, jnp.bfloat16

R = 256
WT = 512
NQ = 4
NW = 2
ORDER = ((1, 0), (1, 1), (1, 2), (0, 0), (1, 3), (0, 1), (0, 2), (0, 3))


def tables(rows):
    half = HEAD // 2
    rate = np.power(np.float32(THETA), -np.arange(half, dtype=np.float32) / np.float32(half)).astype(np.float32)
    angle = np.arange(rows, dtype=np.float32)[:, None] * rate
    cos, sin = np.cos(angle), np.sin(angle)
    return np.concatenate([cos, sin], 1).astype(np.float32)


def kernel(x_ref, gain_ref, table_ref, wq_ref, wk_ref, wv_ref, wo_ref, y_ref, own_ref,
           gain_v, gain_s, xraw, xa, table_s, ring, wring, raw_s, qk_s, v_s, seen, top_s, mix_s,
           dsend, drecv, p1send, p1recv, p2send, p2recv, acc, fin, xres,
           x_sem, gain_sem, t_sem, ring_sem, wring_sem, xres_sem,
           d_ss, d_rs, p1_ss, p1_rs, p2_ss, p2_rs, p3_ss, p3_rs, p4_ss, p4_rs, p4f_ss, p4f_rs,
           loc_sem, e2_ss, e3_ss, e4_ss, e_rs):
    rows, width = x_ref.shape
    nc = rows // R
    heads = v_s.shape[0]
    cols = heads * HEAD
    half = width // 2
    tile = half // 4
    piece = tile // 2
    steps = cols // WT
    deep = width // 2
    quarter_rows = R // 4

    me = lax.axis_index("tp")
    core, yy, xx = lax.rem(me, 2), lax.rem(me // 2, 2), me // 4
    mate = me + 1 - 2 * core
    ypeer = me + 2 - 4 * yy
    xpeer = me + 4 - 8 * xx
    peers = (xpeer, ypeer)
    cross = (ypeer, xpeer)

    def remote(src, dst, ss, rs, to):
        return pltpu.make_async_remote_copy(src, dst, ss, rs, device_id={"tp": to}, device_id_type=MESH)

    def column(h, kind, s):
        a = kind % 2 == 0
        lead, other = (xx, yy) if a else (yy, xx)
        big = 1 - lead if kind < 2 else lead
        small = other if s == 0 else 1 - other
        return pl.multiple_of(h * half + (0 if a else 2 * tile) + big * tile + small * piece, piece)

    def at_rows(c):
        return pl.ds(pl.multiple_of(c * R, R), R)

    def x_copies(c):
        return [pltpu.make_async_copy(x_ref.at[pl.ds(pl.multiple_of(c * R + b * quarter_rows, quarter_rows), quarter_rows)],
                                      xraw.at[pl.ds(b * quarter_rows, quarter_rows)], x_sem.at[b]) for b in range(4)]

    def tile_copy(w, t, f):
        return pltpu.make_async_copy(w.at[pl.ds(f * deep, deep), pl.ds(pl.multiple_of(t * WT, WT), WT)], ring.at[2 * t + f], ring_sem.at[2 * t + f])

    def wo_copies(n, slot):
        mate_half, kind = ORDER[n]
        h = 1 - core if mate_half else core
        return [pltpu.make_async_copy(wo_ref.at[:, pl.ds(column(h, kind, s), piece)],
                                      wring.at[slot, :, pl.ds(s * piece, piece)], wring_sem.at[slot, s]) for s in range(2)]

    def d_copy(c, k):
        p = lax.rem(c, 2)
        return remote(dsend.at[k], drecv.at[p, k], d_ss.at[k], d_rs.at[p, k], mate)

    def p1_copy(c, k):
        p = lax.rem(c, 2)
        return remote(p1send.at[k], p1recv.at[k], p1_ss.at[k], p1_rs.at[p, k], peers[k])

    def p2_copy(c, k):
        p = lax.rem(c, 2)
        return remote(p2send.at[k], p2recv.at[p, k], p2_ss.at[k], p2_rs.at[p, k], cross[k])

    def mine(c, k):
        return y_ref.at[at_rows(c), pl.ds(column(core, 2 + k, 0), piece)]

    def p3_copy(c, k):
        p = lax.rem(c, 2)
        return remote(fin.at[p, k], mine(c, k), p3_ss.at[p, k], p3_rs.at[p, k], cross[k])

    def p4_copy(c, k):
        p = lax.rem(c, 2)
        return remote(fin.at[p, k], mine(c, k), p4_ss.at[p, k], p4_rs.at[p, k], peers[k])

    def e2_copy(c, k):
        p = lax.rem(c, 2)
        return remote(fin.at[p, k], mine(c, k), e2_ss.at[p, k], e_rs, mate)

    def loc_copy(c, k):
        p = lax.rem(c, 2)
        return pltpu.make_async_copy(fin.at[p, k], mine(c, k), loc_sem.at[p, k])

    def own_copy(k):
        p = (nc - 1) % 2
        return pltpu.make_async_copy(fin.at[p, k], own_ref.at[k], loc_sem.at[p, k])

    def came3(c, k):
        return y_ref.at[at_rows(c), pl.ds(column(core, 2 + k, 1), piece)]

    def p4f_copy(c, k):
        p = lax.rem(c, 2)
        return remote(came3(c, k), came3(c, k), p4f_ss.at[p, k], p4f_rs.at[p, k], peers[k])

    def e3_copy(c, k):
        p = lax.rem(c, 2)
        return remote(came3(c, k), came3(c, k), e3_ss.at[p, k], e_rs, mate)

    def e4_copy(c, k):
        p = lax.rem(c, 2)
        lead = xx if k == 0 else yy
        first = pl.multiple_of(core * half + 2 * k * tile + (1 - lead) * tile, tile)
        there = y_ref.at[at_rows(c), pl.ds(first, tile)]
        return remote(there, there, e4_ss.at[p, k], e_rs, mate)

    def norm(first, count):
        lanes = [slice(n, n + HEAD) for n in range(0, width, HEAD)]
        for b in range(count):
            at = pl.ds(pl.multiple_of(first + b * 16, 16), 16)
            squares = [jnp.zeros((16, HEAD), F32)] * 4
            for n, lane in enumerate(lanes):
                wide = xraw[at, lane].astype(F32)
                squares[n % 4] += wide * wide
            total = jnp.sum(sum(squares[1:], squares[0]), -1, keepdims=True)
            scale = lax.rsqrt(total * (1 / width) + 1e-6)
            for lane in lanes:
                xa[at, lane] = (xraw[at, lane].astype(F32) * scale * gain_s[:, lane]).astype(BF16)

    gains = pltpu.make_async_copy(gain_ref, gain_v, gain_sem)
    gains.start()
    for copy in x_copies(0):
        copy.start()
    tile_copy(wq_ref, 0, 0).start()
    barrier = pltpu.get_barrier_semaphore()
    for to in (mate, xpeer, ypeer):
        pl.semaphore_signal(barrier, inc=1, device_id={"tp": to}, device_id_type=MESH)
    for t, f in ((0, 1), (1, 0), (1, 1)):
        tile_copy(wq_ref, t, f).start()
    turns = pltpu.make_async_copy(table_ref, table_s, t_sem)
    turns.start()
    gains.wait()
    gain_s[...] = jnp.broadcast_to(gain_v[...].astype(F32).reshape(1, width), gain_s.shape)

    def some(b, _):
        pltpu.make_async_copy(x_ref.at[pl.ds(0, quarter_rows)], xraw.at[pl.ds(b * quarter_rows, quarter_rows)], x_sem.at[b]).wait()
        norm(b * quarter_rows, quarter_rows // 16)
        return 0

    lax.fori_loop(0, 4, some, 0)
    v_s[:, HEAD:, :] = jnp.ones((heads, 8, rows), BF16)
    turns.wait()

    def store_turned(i, j):
        here = at_rows(i)
        kind, t = j // steps, lax.rem(j, steps)
        both = table_s[here, :]
        other = pltpu.roll(both, HEAD // 2, 1)
        low = lax.broadcasted_iota(jnp.int32, both.shape, 1) < HEAD // 2
        cos, sin = jnp.where(low, both, other), jnp.where(low, -other, both)
        for n in range(WT // HEAD):
            h = t * (WT // HEAD) + n
            one_head = raw_s[:, n * HEAD:(n + 1) * HEAD].astype(F32)
            turned = (one_head * cos + pltpu.roll(one_head, HEAD // 2, 1) * sin).astype(BF16)
            to = kind * (h * rows + i * R) + (1 - kind) * (heads * rows + h * R)
            qk_s[pl.ds(pl.multiple_of(to, R), R), :] = turned

    def store_values(i, t):
        for n in range(WT // HEAD):
            v_s[t * (WT // HEAD) + n, pl.ds(0, HEAD), at_rows(i)] = raw_s[:, n * HEAD:(n + 1) * HEAD].T

    def step(t, store, follow):
        for f in range(2):
            pltpu.make_async_copy(wq_ref.at[pl.ds(0, deep), pl.ds(0, WT)], ring.at[2 * t + f], ring_sem.at[2 * t + f]).wait()
        store()
        out = jnp.dot(xa[:, :deep], ring[2 * t], preferred_element_type=F32)
        raw_s[...] = (out + jnp.dot(xa[:, deep:], ring[2 * t + 1], preferred_element_type=F32)).astype(BF16)
        for f in range(2):
            follow(f)

    def queries_keys(i):
        def one(j, _):
            t = lax.rem(j, steps)

            def follow(f):
                for n, w in enumerate((wk_ref, wv_ref)):
                    @pl.when(j // steps == n)
                    def _():
                        tile_copy(w, t, f).start()

            step(t, lambda: store_turned(i, jnp.maximum(j - 1, 0)), follow)
            return 0

        lax.fori_loop(0, 2 * steps, one, 0)

    def values(i):
        for t in range(steps):
            def follow(f):
                @pl.when(i + 1 < nc)
                def _():
                    tile_copy(wq_ref, t, f).start()

            step(t, (lambda: store_turned(i, 2 * steps - 1)) if t == 0 else (lambda: store_values(i, t - 1)), follow)
        store_values(i, steps - 1)

    def attention(i):
        e = HEAD**-0.5 * LOG2E
        for h in range(heads):
            top_s[h:h + 1, :] = jnp.full((1, R), NEG, F32)
            mix_s[h] = jnp.zeros((HEAD + 8, R), F32)

        def block(j, nk, masked):
            here = pl.ds(pl.multiple_of(j * R, R), nk * R)

            def score(h):
                keys = qk_s[pl.ds(pl.multiple_of(h * rows + j * R, R), nk * R), :]
                queries = qk_s[heads * rows + h * R:heads * rows + (h + 1) * R, :]
                return lax.dot_general(keys, queries, (((1,), (1,)), ((), ())), preferred_element_type=F32)

            def mix(h, weight, keep):
                mix_s[h] = mix_s[h] * keep + jnp.dot(v_s[h, :, here], weight, preferred_element_type=F32)

            if masked:
                ok = lax.broadcasted_iota(jnp.int32, (nk * R, R), 1) + (nk - 1) * R >= lax.broadcasted_iota(jnp.int32, (nk * R, R), 0)
            def soft(h, s):
                if masked:
                    s = jnp.where(ok, s, HIDDEN)
                old = top_s[h:h + 1, :]
                top = jnp.maximum(old, s.max(axis=0, keepdims=True))
                top_s[h:h + 1, :] = top
                return jnp.exp2((s - top) * e).astype(BF16), jnp.exp2((old - top) * e)
            scores = [score(h) for h in range(heads)]
            ws = [soft(h, scores[h]) for h in range(heads)]
            for h in range(heads):
                mix(h, *ws[h])

        def whole(j, _):
            block(j * 2, 2, False)
            return 0

        lax.fori_loop(0, i // 2, whole, 0)

        @pl.when(lax.rem(i, 2) == 0)
        def _():
            block(i, 1, True)

        @pl.when(lax.rem(i, 2) == 1)
        def _():
            block(i - 1, 2, True)

        for h in range(heads):
            total = mix_s[h, HEAD:HEAD + 1, :]
            seen[:, h * HEAD:(h + 1) * HEAD] = (mix_s[h, :HEAD, :] * (1 / total)).T.astype(BF16)

    def output(i):
        p = lax.rem(i, 2)

        @pl.when(i + 1 < nc)
        def _():
            for copy in x_copies(i + 1):
                copy.wait()

        for n, (mate_half, k) in enumerate(ORDER):
            slot = lax.rem(i * 8 + n, NW)
            for copy in wo_copies(n, slot):
                copy.wait()
            if not mate_half:
                d_copy(i, k).wait_recv()
            norm(n * (R // 8), R // 8 // 16)
            out = jnp.dot(seen[...], wring[slot], preferred_element_type=F32)
            if mate_half:
                dsend[k] = out.astype(BF16)
            elif k < 2:
                p1send[k] = (out + drecv[p, k].astype(F32)).astype(BF16)
            else:
                acc[k - 2] = out + drecv[p, k].astype(F32)
            after = n + NW
            if after < 8:
                for copy in wo_copies(after, slot):
                    copy.start()
            else:
                @pl.when(i + 1 < nc)
                def _():
                    for copy in wo_copies(after - 8, slot):
                        copy.start()
            if mate_half:
                d_copy(i, k).start()
            elif k < 2:
                p1_copy(i, k).start()

        @pl.when(i + 2 < nc)
        def _():
            for copy in x_copies(i + 2):
                copy.start()

    def xres_copy(c, k):
        return pltpu.make_async_copy(x_ref.at[at_rows(c), pl.ds(column(core, 2 + k, 0), piece)], xres.at[k], xres_sem.at[k])

    def second(c):
        p = lax.rem(c, 2)
        for k in range(4):
            d_copy(c, k).wait_send()
        for k in range(2):
            p1_copy(c, k).wait()
            xres_copy(c, k).start()

            @pl.when(c > 0)
            def _():
                p2_copy(c - 1, k).wait_send()
        for k in range(2):
            p2send[k] = (acc[k, :, piece:] + p1recv[k, :, piece:].astype(F32)).astype(BF16)
            acc[k, :, :piece] = acc[k, :, :piece] + p1recv[k, :, :piece].astype(F32)
        for k in range(2):
            p2_copy(c, k).start()

    def third(c):
        p = lax.rem(c, 2)

        @pl.when(c >= 2)
        def _():
            done_fin(c - 2)

        for k in range(2):
            p2_copy(c, k).wait_recv()
            xres_copy(c, k).wait()
        for k in range(2):
            fin[p, k] = (acc[k, :, :piece] + p2recv[p, k].astype(F32) + xres[k].astype(F32)).astype(BF16)

        @pl.when(c < nc - 1)
        def _():
            for k in range(2):
                p3_copy(c, k).start()
            for k in range(2):
                loc_copy(c, k).start()
                e2_copy(c, k).start()

        @pl.when(c == nc - 1)
        def _():
            for k in range(2):
                own_copy(k).start()

    def done_fin(c):
        for k in range(2):
            p3_copy(c, k).wait_send()
            p4_copy(c, k).wait_send()
            e2_copy(c, k).wait_send()
            loc_copy(c, k).wait()

    def done_fwd(c):
        for k in range(2):
            p4f_copy(c, k).wait_send()
            e3_copy(c, k).wait_send()

    def forward(c):
        @pl.when(c >= 2)
        def _():
            done_fwd(c - 2)

        for k in range(2):
            p3_copy(c, k).wait_recv()
            p4f_copy(c, k).start()
        for k in range(2):
            e3_copy(c, k).start()

    def last(c):
        @pl.when(c >= 2)
        def _():
            for k in range(2):
                e4_copy(c - 2, k).wait_send()

        for k in range(2):
            p4_copy(c, k).wait_recv()
            p4f_copy(c, k).wait_recv()
            e4_copy(c, k).start()

    def iteration(i, _):
        @pl.when(i < nc)
        def _():
            queries_keys(i)

        @pl.when(i == 0)
        def _():
            pl.semaphore_wait(barrier, 3)
            for n in range(NW):
                for copy in wo_copies(n, n):
                    copy.start()
            for copy in x_copies(1):
                copy.start()

        @pl.when(i == nc)
        def _():
            forward(nc - 2)

        @pl.when(i >= 1)
        def _():
            second(i - 1)

        @pl.when((i >= 2) & (i < nc))
        def _():
            forward(i - 2)

        @pl.when(i < nc)
        def _():
            values(i)
            attention(i)

        @pl.when(i == nc)
        def _():
            last(nc - 2)

        @pl.when(i >= 1)
        def _():
            third(i - 1)

        @pl.when(i < nc)
        def _():
            output(i)

        @pl.when((i >= 1) & (i < nc))
        def _():
            for k in range(2):
                p4_copy(i - 1, k).start()

        @pl.when((i >= 2) & (i < nc))
        def _():
            last(i - 2)

        return 0

    lax.fori_loop(0, nc + 1, iteration, 0)

    done_fin(nc - 2)
    for k in range(2):
        p2_copy(nc - 1, k).wait_send()
        own_copy(k).wait()
    for c in (nc - 3, nc - 2):
        done_fwd(c)
        for k in range(2):
            e4_copy(c, k).wait_send()
    theirs = y_ref.at[pl.ds(0, (nc - 1) * R), pl.ds(pl.multiple_of((1 - core) * half, half), half)]
    remote(theirs, theirs, e2_ss.at[0, 0], e_rs, mate).wait_recv()


FIRST, SECOND = 1152, 512
SLOTS, AHEAD, STRIP = 12, 6, 64


def moved(y, into, first, count):
    width = y.shape[1]
    n = count // STRIP

    def body(*refs):
        src, dst, buf, in_sem, out_sem = refs[0], *refs[-4:]

        def rows_of(j):
            return pl.ds(pl.multiple_of(first + j * STRIP, STRIP), STRIP)

        def read(j):
            slot = lax.rem(j, SLOTS)
            return pltpu.make_async_copy(src.at[rows_of(j)], buf.at[slot], in_sem.at[slot])

        def write(j):
            slot = lax.rem(j, SLOTS)
            return pltpu.make_async_copy(buf.at[slot], dst.at[rows_of(j)], out_sem.at[slot])

        for j in range(min(AHEAD, n)):
            read(jnp.int32(j)).start()

        def one(j, _):
            read(j).wait()
            write(j).start()

            @pl.when((j + AHEAD < n) & (j + AHEAD >= SLOTS))
            def _():
                write(j + AHEAD - SLOTS).wait()

            @pl.when(j + AHEAD < n)
            def _():
                read(j + AHEAD).start()
            return 0

        lax.fori_loop(0, n, one, 0)
        for j in range(max(n - SLOTS, 0), n):
            write(jnp.int32(j)).wait()

    given = (y,) if into is None else (y, into)
    return pl.pallas_call(
        body,
        out_shape=jax.ShapeDtypeStruct(y.shape, y.dtype),
        in_specs=[pl.BlockSpec(memory_space=pl.ANY)] * len(given),
        out_specs=pl.BlockSpec(memory_space=pl.ANY),
        scratch_shapes=[pltpu.VMEM((SLOTS, STRIP, width), BF16), pltpu.SemaphoreType.DMA((SLOTS,)), pltpu.SemaphoreType.DMA((SLOTS,))],
        input_output_aliases={} if into is None else {1: 0},
        cost_estimate=pl.CostEstimate(flops=0, transcendentals=0, bytes_accessed=4 * count * width),
        name="moved%d" % first,
    )(*given)


def placed(y, halves):
    rows, width = y.shape
    piece, tile, half = width // 16, width // 8, width // 2

    def body(*refs):
        dst, buf, in_sem, out_sem = refs[-4:]
        me = lax.axis_index("tp")
        core, yy, xx = lax.rem(me, 2), lax.rem(me // 2, 2), me // 4
        reads, writes = [], []
        for n in range(2):
            own, from_y, from_x, far_a, far_b = refs[1 + 5 * n:6 + 5 * n]
            base = (core if n == 0 else 1 - core) * half
            for src, b, big, small in ((own.at[0], 0, xx, yy), (from_y.at[0], 0, xx, 1 - yy), (from_x.at[0], 0, 1 - xx, yy),
                                       (far_a, 0, 1 - xx, 1 - yy), (own.at[1], 1, yy, xx), (from_x.at[1], 1, yy, 1 - xx),
                                       (from_y.at[1], 1, 1 - yy, xx), (far_b, 1, 1 - yy, 1 - xx)):
                at = len(reads)
                to = pl.multiple_of(base + 2 * b * tile + big * tile + small * piece, piece)
                reads.append(pltpu.make_async_copy(src, buf.at[at], in_sem.at[at]))
                writes.append(pltpu.make_async_copy(buf.at[at], dst.at[pl.ds(rows - R, R), pl.ds(to, piece)], out_sem.at[at]))
        for copy in reads:
            copy.start()
        for read, write in zip(reads, writes):
            read.wait()
            write.start()
        for copy in writes:
            copy.wait()

    given = (y, *halves[0], *halves[1])
    return pl.pallas_call(
        body,
        out_shape=jax.ShapeDtypeStruct(y.shape, y.dtype),
        in_specs=[pl.BlockSpec(memory_space=pltpu.HBM)] * len(given),
        out_specs=pl.BlockSpec(memory_space=pltpu.HBM),
        scratch_shapes=[pltpu.VMEM((16, R, piece), BF16), pltpu.SemaphoreType.DMA((16,)), pltpu.SemaphoreType.DMA((16,))],
        input_output_aliases={0: 0},
        cost_estimate=pl.CostEstimate(flops=0, transcendentals=0, bytes_accessed=4 * R * width),
    )(*given)


def solution(mesh):
    def step(x, gain, wq, wk, wv, wo):
        rows, width = x.shape
        cols = wq.shape[1]
        heads = cols // HEAD
        half, tile, piece = width // 2, width // 8, width // 16
        hbm = pl.BlockSpec(memory_space=pl.ANY)
        dma = pltpu.SemaphoreType.DMA
        scratch = [
            pltpu.VMEM((width,), BF16), pltpu.VMEM((16, width), F32),
            pltpu.VMEM((R, width), BF16), pltpu.VMEM((R, width), BF16),
            pltpu.VMEM((rows, HEAD), F32),
            pltpu.VMEM((NQ, width // 2, WT), BF16), pltpu.VMEM((NW, cols, tile), BF16),
            pltpu.VMEM((R, WT), BF16), pltpu.VMEM((heads * (rows + R), HEAD), BF16), pltpu.VMEM((heads, HEAD + 8, rows), BF16),
            pltpu.VMEM((R, cols), BF16), pltpu.VMEM((heads, R), F32), pltpu.VMEM((heads, HEAD + 8, R), F32),
            pltpu.VMEM((4, R, tile), BF16), pltpu.VMEM((2, 4, R, tile), BF16),
            pltpu.VMEM((2, R, tile), BF16), pltpu.VMEM((2, R, tile), BF16),
            pltpu.VMEM((2, R, piece), BF16), pltpu.VMEM((2, 2, R, piece), BF16),
            pltpu.VMEM((2, R, tile), F32), pltpu.VMEM((2, 2, R, piece), BF16), pltpu.VMEM((2, R, piece), BF16),
            dma((4,)), dma, dma, dma((NQ,)), dma((NW, 2)), dma((2,)),
            dma((4,)), dma((2, 4)),
            dma((2,)), dma((2, 2)),
            dma((2,)), dma((2, 2)),
            dma((2, 2)), dma((2, 2)),
            dma((2, 2)), dma((2, 2)),
            dma((2, 2)), dma((2, 2)),
            dma((2, 2)), dma((2, 2)), dma((2, 2)), dma((2, 2)), dma,
        ]
        most, own = pl.pallas_call(
            kernel,
            out_shape=[jax.ShapeDtypeStruct((rows, width), BF16), jax.ShapeDtypeStruct((2, R, piece), BF16)],
            in_specs=[hbm] * 7,
            out_specs=[hbm, hbm],
            scratch_shapes=scratch,
            compiler_params=pltpu.CompilerParams(collective_id=0, has_side_effects=True, vmem_limit_bytes=67043328),
        )(x, gain, jnp.asarray(tables(rows)), wq, wk, wv, wo)

        def sent(t, bit):
            return lax.ppermute(t, "tp", [(d, d ^ bit) for d in range(8)])

        to_mate, to_y, to_x = 1, 2, 4
        from_y, from_x = sent(own, to_y), sent(own, to_x)
        mates = [sent(own, to_mate)]
        y = moved(most, None, 0, FIRST)
        y, from_y, from_x = lax.optimization_barrier((y, from_y, from_x))
        far = [sent(from_y[0], to_x), sent(from_x[1], to_y)]
        mates += [sent(from_y, to_mate), sent(from_x, to_mate)]
        y = moved(most, y, FIRST, SECOND)
        y, *far = lax.optimization_barrier((y, *far))
        mates += [sent(t, to_mate) for t in far]
        y = moved(most, y, FIRST + SECOND, rows - R - FIRST - SECOND)
        return placed(y, ([own, from_y, from_x, *far], mates))

    tokens, columns = P("dp", None), P(None, "tp")
    return jax.shard_map(
        step,
        mesh=mesh,
        in_specs=(tokens, P(None), columns, columns, columns, P("tp", None)),
        out_specs=tokens,
        check_vma=False,
    )
```
